32 devices in a mesh: ell: 4 (over y, x), blk: 8 (over z, core).
Axes of the slice: x: 2, y: 2, z: 4, core: 2. Of those that a mesh axis runs over, the one named last changes fastest.
Arguments:
- wigner: bfloat16 [8, 17, 2101248], P(None, None, ('ell', 'blk')), may hold values from -6 to 6
- sky_alm: float32 [2, 2101248], P(None, ('ell', 'blk')), may hold values from -0.03125 to 0.03125
- beam_blm: float32 [2, 17, 2048], replicated, may hold values from -4.25 to 4.25
- slot_col: int32 [2101248], P(('ell', 'blk')), may hold values from -1 to 255, as said below
- slot_ell: int32 [2101248], P(('ell', 'blk')), may hold values from 0 to 2047, as said below
- order_of_column: int32 [2048], replicated, may hold values from 0 to 2047, as said below
Outputs:
- conv_cube: float32 [8, 32, 4096], P('ell', 'blk')
The draws below stay inside these ranges and needn't reach their ends.
Inputs may be any that keep to these rules, and one draw needn't show every extreme that they name: `slot_col`: slot block b (slots b * 65664 to b * 65664 + 65663) belongs to ell index b // 8 and blk index b % 8; at most 65568 slots of a block are live, and some blocks have exactly that many. `slot_ell`: every pair (l, m) with m <= l < 2048 stands in exactly one live slot; within a blk group, higher ell indices hold degrees no lower than those of lower ell indices. `order_of_column`: A permutation of 0 to 2047; every blk group's orders hold the same number of pairs.
All inputs are finite; a program needn't handle non-finite values.
Results may differ from the reference program's by a relative error of at most 0.0029.
Values sent between devices are 32-bit elements; how exact they have to be, the bound alone decides.
A program may use at most 256 MiB of HBM per device.

```python
import math
import jax
import jax.numpy as jnp
from jax import lax

L = 2048
K = 17
NPSI = 32
THETA = 8
NPHI = 4096
M_DEV = 256
LIVE_MOST = 65568
SLOT_DEV = 65664
SLOTS = 2101248
N_ELL = 4
N_BLK = 8


def pair_tables(key):
    half = L // 2
    fold = L // (2 * N_BLK)
    blocks = N_ELL * N_BLK
    cols = L // N_BLK
    order = jax.random.permutation(jax.random.fold_in(key, 101), half)
    lower = order.reshape(N_BLK, fold)
    grouped = jnp.concatenate([lower, L - 1 - lower], axis=1).astype(jnp.int32)
    col_keys = jax.random.split(jax.random.fold_in(key, 102), N_BLK)
    col_perm = jax.vmap(lambda inner_key: jax.random.permutation(inner_key, cols))(col_keys)
    order_table = jnp.take_along_axis(grouped, col_perm.astype(jnp.int32), axis=1)
    degrees = jnp.arange(L, dtype=jnp.int32)
    valid = order_table[:, None, :] <= degrees[None, :, None]
    flat_valid = valid.reshape(N_BLK, L * cols)
    position = jnp.cumsum(flat_valid.astype(jnp.int32), axis=1) - 1
    ell_index = position // LIVE_MOST
    offset = jnp.clip(position % LIVE_MOST, 0, SLOT_DEV - 1)
    group_index = jnp.arange(N_BLK, dtype=jnp.int32)[:, None]
    block = jnp.clip(ell_index * N_BLK + group_index, 0, blocks - 1)
    shuffle_keys = jax.random.split(jax.random.fold_in(key, 103), blocks)
    shuffles = jax.vmap(lambda inner_key: jax.random.permutation(inner_key, SLOT_DEV))(shuffle_keys).astype(jnp.int32)
    slot = block * SLOT_DEV + shuffles[block, offset]
    target = jnp.where(flat_valid, slot, blocks * SLOT_DEV).reshape(-1)
    col_values = jnp.broadcast_to(jnp.arange(cols, dtype=jnp.int32)[None, None, :], (N_BLK, L, cols)).reshape(-1)
    ell_values = jnp.broadcast_to(degrees[None, :, None], (N_BLK, L, cols)).reshape(-1)
    slot_col = jnp.full((blocks * SLOT_DEV,), -1, jnp.int32).at[target].set(col_values, mode='drop')
    slot_ell = jnp.zeros((blocks * SLOT_DEV,), jnp.int32).at[target].set(ell_values, mode='drop')
    return (order_table.reshape(L), slot_col, slot_ell)


def draw_order_of_column(key, part):
    return pair_tables(key)[0]


def draw_slot_col(key, part):
    return pair_tables(key)[1]


def draw_slot_ell(key, part):
    return pair_tables(key)[2]


def draw_beam_blm(key, part):
    degrees = jnp.arange(L, dtype=jnp.float32)
    scale = (2.0 * (degrees + 1.0)) ** (-0.5)
    base = jnp.clip(jax.random.normal(key, (2, K, L), jnp.float32), -6.0, 6.0)
    return (base * scale[None, None, :]).astype(jnp.float32)


def level_of(key, shape, pieces, low, top_value):
    def one(dim, blocks):
        draws = jax.random.uniform(jax.random.fold_in(jax.random.fold_in(key, 6), dim), (blocks,), jnp.float32, low / len(pieces), top_value / len(pieces))
        return jnp.repeat(jnp.exp(draws), shape[dim] // blocks).reshape((-1,) + (1,) * (len(shape) - dim - 1))

    gain = one(*pieces[0])
    for cut in pieces[1:]:
        gain = gain * one(*cut)
    return gain


def scatter_about(rng, shape, deviation, reach, shards=(), held_as=jnp.bfloat16):
    array = jax.random.normal(rng, shape, jnp.float32) * deviation
    if len(shards) > 0:
        array = level_of(rng, shape, shards, -0.22, 0.18) * array
    return jnp.clip(array, min=-reach, max=reach).astype(held_as)


def setup_inputs(seed: int = 0) -> dict:
    key_of = jax.random.split(jax.random.key(seed), 7)
    wigner = scatter_about(key_of[0], (THETA, K, SLOTS), 1.0, 6.0, ((2, 32),))
    sky_alm = scatter_about(key_of[1], (2, SLOTS), (L * K) ** -0.5, 0.03125, ((1, 32),), jnp.float32)
    beam_blm = draw_beam_blm(jax.random.fold_in(key_of[6], 71), 0)
    slot_col = draw_slot_col(jax.random.fold_in(key_of[6], 71), 0)
    slot_ell = draw_slot_ell(jax.random.fold_in(key_of[6], 71), 0)
    order_of_column = draw_order_of_column(jax.random.fold_in(key_of[6], 71), 0)
    return dict(wigner=wigner, sky_alm=sky_alm, beam_blm=beam_blm, slot_col=slot_col, slot_ell=slot_ell, order_of_column=order_of_column)


def phase_table(rows, cols, period):
    product = (jnp.arange(rows, dtype=jnp.int32)[:, None] * jnp.arange(cols, dtype=jnp.int32)[None, :]) % period
    angle = product.astype(jnp.float32) * (2.0 * math.pi / period)
    return jnp.cos(angle), jnp.sin(angle)


def psi_table(order_count, samples):
    cosines, sine_terms = phase_table(order_count, samples, samples)
    real_row = jnp.stack([cosines, sine_terms], axis=1)
    imag_row = jnp.stack([-sine_terms, cosines], axis=1)
    return jnp.stack([real_row, imag_row], axis=0)


def reference(wigner, sky_alm, beam_blm, slot_col, slot_ell, order_of_column):
    block_count = SLOTS // SLOT_DEV

    def accumulate(running, block_index):
        first_slot = block_index * SLOT_DEV
        wig_rows = lax.dynamic_slice_in_dim(wigner, first_slot, SLOT_DEV, 2).astype(jnp.float32)
        alm_part = lax.dynamic_slice_in_dim(sky_alm, first_slot, SLOT_DEV, 1)
        columns = lax.dynamic_slice_in_dim(slot_col, first_slot, SLOT_DEV, 0)
        degrees = lax.dynamic_slice_in_dim(slot_ell, first_slot, SLOT_DEV, 0)
        beam_slots = jnp.take(beam_blm, degrees, axis=2)
        coeffs = jnp.stack([alm_part[0] * beam_slots[0] - alm_part[1] * beam_slots[1],
                            alm_part[0] * beam_slots[1] + alm_part[1] * beam_slots[0]])
        values = (wig_rows[:, None] * coeffs[None]).astype(jnp.bfloat16)
        values = lax.optimization_barrier(values).astype(jnp.float32)
        group = (block_index % N_BLK).astype(jnp.int32)
        global_col = group * M_DEV + jnp.maximum(columns, 0)
        orders = jnp.where(columns >= 0, jnp.take(order_of_column, global_col), L).astype(jnp.int32)
        flat = values.reshape(THETA * 2 * K, SLOT_DEV).T
        return running + jax.ops.segment_sum(flat, orders, num_segments=L + 1)[:L], None

    totals, _ = lax.scan(accumulate, jnp.zeros((L, THETA * 2 * K), jnp.float32),
                         jnp.arange(block_count, dtype=jnp.int32))
    harmonic = totals.T.reshape(THETA, 2, K, L)
    psi_field = jnp.einsum("trkc,rksp->tspc", harmonic, psi_table(K, NPSI), precision=lax.Precision.HIGHEST)
    complex_field = psi_field[:, 0] + 1j * psi_field[:, 1]
    padded = jnp.pad(complex_field, ((0, 0), (0, 0), (0, NPHI - L)))
    return (jnp.real(jnp.fft.ifft(padded, axis=-1)) * NPHI).astype(jnp.float32)
```

```python
import functools
import math

import jax
import jax.numpy as jnp
from jax import lax
from jax.experimental import pallas as pl
from jax.experimental.pallas import tpu as pltpu
from jax.sharding import PartitionSpec as P

NPSI = 32
LANES = 128
SUBLANES = 8


def phase_table(rows, cols, period):
    product = (
        jnp.arange(rows, dtype=jnp.int32)[:, None]
        * jnp.arange(cols, dtype=jnp.int32)[None, :]
        % period
    )
    angle = product.astype(jnp.float32) * (2.0 * math.pi / period)
    return (jnp.cos(angle), jnp.sin(angle))


def psi_table(order_count, samples):
    cosines, sine_terms = phase_table(order_count, samples, samples)
    real_row = jnp.stack([cosines, sine_terms], axis=1)
    imag_row = jnp.stack([-sine_terms, cosines], axis=1)
    return jnp.stack([real_row, imag_row], axis=0)


def to_phi(fields, order_of_column):
    cycles = fields.shape[0]
    samples = fields.shape[2]
    degrees = fields.shape[3]
    period = 2 * degrees
    inner = 2 ** ((period.bit_length() - 1) // 2)
    outer = period // inner
    highest = lax.Precision.HIGHEST
    high_part = order_of_column // inner
    low_part = order_of_column % inner
    turns = high_part[:, None] * jnp.arange(outer, dtype=jnp.int32)[None, :] % outer
    angle = turns.astype(jnp.float32) * (2.0 * math.pi / outer)
    cos_first = jnp.cos(angle)
    sin_first = jnp.sin(angle)
    select = (low_part[:, None] == jnp.arange(inner, dtype=jnp.int32)[None, :]).astype(jnp.float32)
    real_in = fields[:, 0]
    imag_in = fields[:, 1]
    weighted_re = real_in[..., None] * cos_first - imag_in[..., None] * sin_first
    weighted_im = real_in[..., None] * sin_first + imag_in[..., None] * cos_first
    first_re = jnp.einsum("tpcj,cv->tpvj", weighted_re, select, precision=highest)
    first_im = jnp.einsum("tpcj,cv->tpvj", weighted_im, select, precision=highest)
    cos_twist, sin_twist = phase_table(inner, outer, period)
    twist_re = first_re * cos_twist - first_im * sin_twist
    twist_im = first_re * sin_twist + first_im * cos_twist
    cos_last, sin_last = phase_table(inner, inner, inner)
    result = jnp.einsum("tpvj,vw->tpwj", twist_re, cos_last, precision=highest) - jnp.einsum(
        "tpvj,vw->tpwj", twist_im, sin_last, precision=highest
    )
    return result.reshape(cycles, samples, period)


def largest_part(total, most):
    return max(part for part in range(1, total + 1) if total % part == 0 and part <= most)


def beam_table(beam):
    orders, degrees = beam.shape[1], beam.shape[2]
    whole = orders // SUBLANES * SUBLANES
    rest = orders - whole
    rows = [beam[0, :whole], beam[1, :whole]]
    if rest > 0:
        real, imag = beam[0, whole:], beam[1, whole:]
        short = SUBLANES // 4 if rest <= SUBLANES // 4 else SUBLANES
        real = jnp.pad(real, ((0, short - rest), (0, 0)))
        imag = jnp.pad(imag, ((0, short - rest), (0, 0)))
        rows += [real, imag, -imag, real] if short < SUBLANES else [real, imag]
    table = jnp.concatenate(rows, axis=0)
    tiles = degrees // LANES
    return table.reshape(table.shape[0], tiles, LANES).transpose(1, 0, 2)


def lane_pick(table, index):
    return lax.gather(
        table,
        index[..., None],
        lax.GatherDimensionNumbers(
            offset_dims=(),
            collapsed_slice_dims=(1,),
            start_index_map=(1,),
            operand_batching_dims=(0,),
            start_indices_batching_dims=(0,),
        ),
        slice_sizes=(1, 1),
        mode=lax.GatherScatterMode.PROMISE_IN_BOUNDS,
    )


def sums_kernel(
    orders, sub, wig_ref, sky_ref, col_ref, ell_ref, table_ref, out_ref, coeff_ref, value_ref, hot_ref
):
    cycles = wig_ref.shape[1]
    chunk = wig_ref.shape[2]
    tiles, rows, _ = table_ref.shape
    groups = rows // SUBLANES
    whole = orders // SUBLANES
    rest = orders - whole * SUBLANES
    packed = 0 < rest <= SUBLANES // 4
    cols = hot_ref.shape[0]
    parts = sub // LANES

    live = col_ref[...] >= 0
    degree = ell_ref[...]
    top = jnp.max(jnp.where(live, degree, 0).astype(jnp.float32)).astype(jnp.int32) // LANES
    low = jnp.min(jnp.where(live, degree, tiles * LANES - 1).astype(jnp.float32)).astype(jnp.int32) // LANES
    span = top - low + 1

    def pick_all(count, first, start):
        for part in range(parts):
            lanes = pl.ds(pl.multiple_of(start + part * LANES, LANES), LANES)
            ell = jnp.broadcast_to(ell_ref[:, lanes], (SUBLANES, LANES))
            high = (ell >> 7) - first
            index = ell & (LANES - 1)
            picked = [jnp.zeros((SUBLANES, LANES), jnp.float32) for _ in range(groups)]
            for tile in range(count):
                here = high == tile
                for group in range(groups):
                    entry = table_ref[first + tile, pl.ds(group * SUBLANES, SUBLANES), :]
                    picked[group] = jnp.where(here, lane_pick(entry, index), picked[group])
            sky_re = jnp.broadcast_to(sky_ref[0:1, lanes], (SUBLANES, LANES))
            sky_im = jnp.broadcast_to(sky_ref[1:2, lanes], (SUBLANES, LANES))
            out = []
            for group in range(whole):
                out.append(sky_re * picked[group] - sky_im * picked[whole + group])
            for group in range(whole):
                out.append(sky_re * picked[whole + group] + sky_im * picked[group])
            if packed:
                row = lax.broadcasted_iota(jnp.int32, (SUBLANES, LANES), 0)
                term = picked[2 * whole] * jnp.where(row < SUBLANES // 2, sky_re, sky_im)
                out.append(term + pltpu.roll(term, SUBLANES // 2, 0))
            elif rest > 0:
                out.append(sky_re * picked[2 * whole] - sky_im * picked[2 * whole + 1])
                out.append(sky_re * picked[2 * whole + 1] + sky_im * picked[2 * whole])
            here = slice(part * LANES, (part + 1) * LANES)
            for group, block in enumerate(out):
                coeff_ref[pl.ds(group * SUBLANES, SUBLANES), here] = block

    def row_of(part, order):
        if order < whole * SUBLANES:
            return part * whole * SUBLANES + order
        step = SUBLANES // 4 if packed else SUBLANES
        return 2 * whole * SUBLANES + part * step + order - whole * SUBLANES

    def run(count, first):
        @pl.loop(0, chunk // sub)
        def _(step):
            start = pl.multiple_of(step * sub, LANES)
            pick_all(count, first, start)
            lanes = pl.ds(start, sub)
            for order in range(orders):
                wig = wig_ref[order, :, lanes].astype(jnp.float32)
                real = wig * coeff_ref[pl.ds(row_of(0, order), 1), :]
                imag = wig * coeff_ref[pl.ds(row_of(1, order), 1), :]
                both = jnp.concatenate([real, imag], axis=0).astype(jnp.bfloat16)
                value_ref[pl.ds(order * 2 * cycles, 2 * cycles), lanes] = both
            col = jnp.broadcast_to(col_ref[:, lanes], (cols, sub))
            row = lax.broadcasted_iota(jnp.int32, (cols, sub), 0)
            hot_ref[:, lanes] = (row == col).astype(jnp.float32).astype(jnp.bfloat16)

    counts = sorted({min(c, tiles) for c in (4, 5, 9)})
    below = 0
    for count in counts:
        first = jnp.minimum(low, tiles - count)

        @pl.when((span > below) & (span <= count) if below else span <= count)
        def _():
            run(count, first)

        below = count
    if below < tiles:

        @pl.when(span > below)
        def _():
            run(tiles, 0)

    part = lax.dot_general(
        value_ref[...],
        hot_ref[...],
        (((1,), (1,)), ((), ())),
        preferred_element_type=jnp.float32,
    )

    @pl.when(pl.program_id(0) == 0)
    def _():
        out_ref[...] = part

    @pl.when(pl.program_id(0) > 0)
    def _():
        out_ref[...] += part


def order_sums(wigner, sky_alm, beam_blm, slot_col, slot_ell, cols):
    cycles, orders, slots = wigner.shape
    tiles = slots // LANES
    chunk = LANES * largest_part(tiles, 64)
    sub = LANES * largest_part(chunk // LANES, 3)
    table = beam_table(beam_blm)
    rows = orders * 2 * cycles
    return pl.pallas_call(
        functools.partial(sums_kernel, orders, sub),
        out_shape=jax.ShapeDtypeStruct((rows, cols), jnp.float32),
        grid=(slots // chunk,),
        in_specs=[
            pl.BlockSpec((orders, cycles, chunk), lambda i: (0, 0, i)),
            pl.BlockSpec((2, chunk), lambda i: (0, i)),
            pl.BlockSpec((1, chunk), lambda i: (0, i)),
            pl.BlockSpec((1, chunk), lambda i: (0, i)),
            pl.BlockSpec(table.shape, lambda i: (0, 0, 0)),
        ],
        out_specs=pl.BlockSpec((rows, cols), lambda i: (0, 0)),
        scratch_shapes=[
            pltpu.VMEM((table.shape[1], sub), jnp.float32),
            pltpu.VMEM((rows, chunk), jnp.bfloat16),
            pltpu.VMEM((cols, chunk), jnp.bfloat16),
        ],
        compiler_params=pltpu.CompilerParams(
            dimension_semantics=("arbitrary",), vmem_limit_bytes=48 * 1024 * 1024
        ),
        name="order_sums",
    )(wigner.transpose(1, 0, 2), sky_alm, slot_col[None, :], slot_ell[None, :], table)


def on_device(wigner, sky_alm, beam_blm, slot_col, slot_ell, order_of_column):
    cycle_total = wigner.shape[0]
    order_count = wigner.shape[1]
    blk_count = lax.axis_size("blk")
    col_count = order_of_column.shape[0] // blk_count
    col_sums = order_sums(wigner, sky_alm, beam_blm, slot_col, slot_ell, col_count)
    by_cycle = col_sums.reshape(order_count, 2, cycle_total, col_count).transpose(2, 1, 0, 3)
    summed = lax.psum_scatter(by_cycle, "ell", scatter_dimension=0, tiled=True)
    owned = jnp.einsum(
        "trkc,rksp->tspc",
        summed,
        psi_table(order_count, NPSI),
        precision=lax.Precision.HIGHEST,
    )
    return to_phi(
        lax.all_to_all(owned, "blk", split_axis=2, concat_axis=3, tiled=True), order_of_column
    )


def solution(mesh):
    return jax.shard_map(
        on_device,
        mesh=mesh,
        in_specs=(
            P(None, None, ("ell", "blk")),
            P(None, ("ell", "blk")),
            P(),
            P(("ell", "blk")),
            P(("ell", "blk")),
            P(),
        ),
        out_specs=P("ell", "blk", None),
        check_vma=False,
    )
```

```python
import functools
import math

import jax
import jax.numpy as jnp
from jax import lax
from jax.experimental import pallas as pl
from jax.experimental.pallas import tpu as pltpu
from jax.sharding import PartitionSpec as P

NPSI = 32
LANES = 128
SUBLANES = 8


def phase_table(rows, cols, period):
    product = (
        jnp.arange(rows, dtype=jnp.int32)[:, None]
        * jnp.arange(cols, dtype=jnp.int32)[None, :]
        % period
    )
    angle = product.astype(jnp.float32) * (2.0 * math.pi / period)
    return (jnp.cos(angle), jnp.sin(angle))


def psi_table(order_count, samples):
    cosines, sine_terms = phase_table(order_count, samples, samples)
    real_row = jnp.stack([cosines, sine_terms], axis=1)
    imag_row = jnp.stack([-sine_terms, cosines], axis=1)
    return jnp.stack([real_row, imag_row], axis=0)


def to_phi(fields, order_of_column):
    cycles = fields.shape[0]
    samples = fields.shape[2]
    degrees = fields.shape[3]
    period = 2 * degrees
    inner = 2 ** ((period.bit_length() - 1) // 2)
    outer = period // inner
    highest = lax.Precision.HIGH
    high_part = order_of_column // inner
    low_part = order_of_column % inner
    turns = high_part[:, None] * jnp.arange(outer, dtype=jnp.int32)[None, :] % outer
    angle = turns.astype(jnp.float32) * (2.0 * math.pi / outer)
    cos_first = jnp.cos(angle)
    sin_first = jnp.sin(angle)
    select = (low_part[:, None] == jnp.arange(inner, dtype=jnp.int32)[None, :]).astype(jnp.float32)
    real_in = fields[:, 0]
    imag_in = fields[:, 1]
    weighted_re = real_in[..., None] * cos_first - imag_in[..., None] * sin_first
    weighted_im = real_in[..., None] * sin_first + imag_in[..., None] * cos_first
    first_re = jnp.einsum("tpcj,cv->tpvj", weighted_re, select, precision=highest)
    first_im = jnp.einsum("tpcj,cv->tpvj", weighted_im, select, precision=highest)
    cos_twist, sin_twist = phase_table(inner, outer, period)
    twist_re = first_re * cos_twist - first_im * sin_twist
    twist_im = first_re * sin_twist + first_im * cos_twist
    cos_last, sin_last = phase_table(inner, inner, inner)
    result = jnp.einsum("tpvj,vw->tpwj", twist_re, cos_last, precision=highest) - jnp.einsum(
        "tpvj,vw->tpwj", twist_im, sin_last, precision=highest
    )
    return result.reshape(cycles, samples, period)


def largest_part(total, most):
    return max(part for part in range(1, total + 1) if total % part == 0 and part <= most)


def beam_table(beam):
    orders, degrees = beam.shape[1], beam.shape[2]
    whole = orders // SUBLANES * SUBLANES
    rest = orders - whole
    rows = [beam[0, :whole], beam[1, :whole]]
    if rest > 0:
        real, imag = beam[0, whole:], beam[1, whole:]
        short = SUBLANES // 4 if rest <= SUBLANES // 4 else SUBLANES
        real = jnp.pad(real, ((0, short - rest), (0, 0)))
        imag = jnp.pad(imag, ((0, short - rest), (0, 0)))
        rows += [real, imag, -imag, real] if short < SUBLANES else [real, imag]
    table = jnp.concatenate(rows, axis=0)
    tiles = degrees // LANES
    return table.reshape(table.shape[0], tiles, LANES).transpose(1, 0, 2)


def lane_pick(table, index):
    return lax.gather(
        table,
        index[..., None],
        lax.GatherDimensionNumbers(
            offset_dims=(),
            collapsed_slice_dims=(1,),
            start_index_map=(1,),
            operand_batching_dims=(0,),
            start_indices_batching_dims=(0,),
        ),
        slice_sizes=(1, 1),
        mode=lax.GatherScatterMode.PROMISE_IN_BOUNDS,
    )


def sums_kernel(
    orders, sub, wig_ref, sky_ref, col_ref, ell_ref, table_ref, out_ref, *scratch
):
    cycles = wig_ref.shape[1]
    chunk = wig_ref.shape[2]
    tiles, rows, _ = table_ref.shape
    groups = rows // SUBLANES
    whole = orders // SUBLANES
    rest = orders - whole * SUBLANES
    packed = 0 < rest <= SUBLANES // 4
    coeff_refs, value_refs, hot_refs = scratch[0:2], scratch[2:4], scratch[4:6]
    cols = out_ref.shape[1]
    parts = sub // LANES

    live = col_ref[...] >= 0
    degree = ell_ref[...]
    top = jnp.max(jnp.where(live, degree, 0).astype(jnp.float32)).astype(jnp.int32) // LANES
    low = jnp.min(jnp.where(live, degree, tiles * LANES - 1).astype(jnp.float32)).astype(jnp.int32) // LANES
    span = top - low + 1

    def pick_all(count, first, start, coeff_ref):
        for part in range(parts):
            lanes = pl.ds(pl.multiple_of(start + part * LANES, LANES), LANES)
            ell = jnp.broadcast_to(ell_ref[:, lanes], (SUBLANES, LANES))
            high = (ell >> 7) - first
            index = ell & (LANES - 1)
            picked = [jnp.zeros((SUBLANES, LANES), jnp.float32) for _ in range(groups)]
            for tile in range(count):
                here = high == tile
                for group in range(groups):
                    entry = table_ref[first + tile, pl.ds(group * SUBLANES, SUBLANES), :]
                    picked[group] = jnp.where(here, lane_pick(entry, index), picked[group])
            sky_re = jnp.broadcast_to(sky_ref[0:1, lanes], (SUBLANES, LANES))
            sky_im = jnp.broadcast_to(sky_ref[1:2, lanes], (SUBLANES, LANES))
            out = []
            for group in range(whole):
                out.append(sky_re * picked[group] - sky_im * picked[whole + group])
            for group in range(whole):
                out.append(sky_re * picked[whole + group] + sky_im * picked[group])
            if packed:
                row = lax.broadcasted_iota(jnp.int32, (SUBLANES, LANES), 0)
                term = picked[2 * whole] * jnp.where(row < SUBLANES // 2, sky_re, sky_im)
                out.append(term + pltpu.roll(term, SUBLANES // 2, 0))
            elif rest > 0:
                out.append(sky_re * picked[2 * whole] - sky_im * picked[2 * whole + 1])
                out.append(sky_re * picked[2 * whole + 1] + sky_im * picked[2 * whole])
            here = slice(part * LANES, (part + 1) * LANES)
            for group, block in enumerate(out):
                coeff_ref[pl.ds(group * SUBLANES, SUBLANES), here] = block

    def row_of(part, order):
        if order < whole * SUBLANES:
            return part * whole * SUBLANES + order
        step = SUBLANES // 4 if packed else SUBLANES
        return 2 * whole * SUBLANES + part * step + order - whole * SUBLANES

    def run(count, first):
        halves = chunk // sub

        def products(half, which):
            start = pl.multiple_of(half * sub, LANES)
            coeff, value, hot = coeff_refs[which], value_refs[which], hot_refs[which]
            pick_all(count, first, start, coeff)
            lanes = pl.ds(start, sub)
            for order in range(orders):
                wig = wig_ref[order, :, lanes].astype(jnp.float32)
                real = wig * coeff[pl.ds(row_of(0, order), 1), :]
                imag = wig * coeff[pl.ds(row_of(1, order), 1), :]
                both = jnp.concatenate([real, imag], axis=0).astype(jnp.bfloat16)
                value[pl.ds(order * 2 * cycles, 2 * cycles), :] = both
            col = jnp.broadcast_to(col_ref[:, lanes], (cols, sub))
            row = lax.broadcasted_iota(jnp.int32, (cols, sub), 0)
            hot[...] = (row == col).astype(jnp.float32).astype(jnp.bfloat16)

        def add_up(which):
            out_ref[...] += lax.dot_general(
                value_refs[which][...],
                hot_refs[which][...],
                (((1,), (1,)), ((), ())),
                preferred_element_type=jnp.float32,
            )

        products(0, 1)

        @pl.loop(0, (halves - 1) // 2)
        def _(pair):
            add_up(1)
            products(2 * pair + 1, 0)
            add_up(0)
            products(2 * pair + 2, 1)

        add_up(1)
        if halves % 2 == 0:
            products(halves - 1, 0)
            add_up(0)

    @pl.when(pl.program_id(0) == 0)
    def _():
        out_ref[...] = jnp.zeros_like(out_ref)

    counts = sorted({min(c, tiles) for c in (4, 9)})
    below = 0
    for count in counts:
        first = jnp.minimum(low, tiles - count)

        @pl.when((span > below) & (span <= count) if below else span <= count)
        def _():
            run(count, first)

        below = count
    if below < tiles:

        @pl.when(span > below)
        def _():
            run(tiles, 0)


def order_sums(wigner, sky_alm, beam_blm, slot_col, slot_ell, cols):
    cycles, orders, slots = wigner.shape
    tiles = slots // LANES
    chunk = LANES * largest_part(tiles, 64)
    sub = LANES * largest_part(chunk // LANES, 3)
    table = beam_table(beam_blm)
    rows = orders * 2 * cycles
    return pl.pallas_call(
        functools.partial(sums_kernel, orders, sub),
        out_shape=jax.ShapeDtypeStruct((rows, cols), jnp.float32),
        grid=(slots // chunk,),
        in_specs=[
            pl.BlockSpec((orders, cycles, chunk), lambda i: (0, 0, i)),
            pl.BlockSpec((2, chunk), lambda i: (0, i)),
            pl.BlockSpec((1, chunk), lambda i: (0, i)),
            pl.BlockSpec((1, chunk), lambda i: (0, i)),
            pl.BlockSpec(table.shape, lambda i: (0, 0, 0)),
        ],
        out_specs=pl.BlockSpec((rows, cols), lambda i: (0, 0)),
        scratch_shapes=[
            *[pltpu.VMEM((table.shape[1], sub), jnp.float32) for _ in range(2)],
            *[pltpu.VMEM((rows, sub), jnp.bfloat16) for _ in range(2)],
            *[pltpu.VMEM((cols, sub), jnp.bfloat16) for _ in range(2)],
        ],
        compiler_params=pltpu.CompilerParams(
            dimension_semantics=("arbitrary",), vmem_limit_bytes=48 * 1024 * 1024
        ),
        name="order_sums",
    )(wigner.transpose(1, 0, 2), sky_alm, slot_col[None, :], slot_ell[None, :], table)


def on_device(wigner, sky_alm, beam_blm, slot_col, slot_ell, order_of_column):
    cycle_total = wigner.shape[0]
    order_count = wigner.shape[1]
    blk_count = lax.axis_size("blk")
    col_count = order_of_column.shape[0] // blk_count
    col_sums = order_sums(wigner, sky_alm, beam_blm, slot_col, slot_ell, col_count)
    by_cycle = col_sums.reshape(order_count, 2, cycle_total, col_count).transpose(2, 1, 0, 3)
    ell_count = lax.axis_size("ell")
    partials = by_cycle.reshape((ell_count, cycle_total // ell_count) + by_cycle.shape[1:])
    summed = lax.all_to_all(partials, "ell", split_axis=0, concat_axis=0, tiled=True).sum(axis=0)
    owned = jnp.einsum(
        "trkc,rksp->tspc",
        summed,
        psi_table(order_count, NPSI),
        precision=lax.Precision.HIGHEST,
    )
    return to_phi(
        lax.all_to_all(owned, "blk", split_axis=2, concat_axis=3, tiled=True), order_of_column
    )


def solution(mesh):
    return jax.shard_map(
        on_device,
        mesh=mesh,
        in_specs=(
            P(None, None, ("ell", "blk")),
            P(None, ("ell", "blk")),
            P(),
            P(("ell", "blk")),
            P(("ell", "blk")),
            P(),
        ),
        out_specs=P("ell", "blk", None),
        check_vma=False,
    )
```
